256 devices in a mesh: expert: 32 (over y, x, core), dp: 8 (over z).
Axes of the slice: x: 4, y: 4, z: 8, core: 2. Of those that a mesh axis runs over, the one named last changes fastest.
Arguments:
- tokens: bfloat16 [49152, 1024], P(('expert', 'dp')), may hold values from -6 to 6
- grad_out: bfloat16 [49152, 1024], P(('expert', 'dp')), may hold values from -6 to 6
- routes: int32 [49152, 2], P(('expert', 'dp')), may hold values from 0 to 31, all different within a row
- keep_second: int32 [49152], P(('expert', 'dp')), may hold values 0 or 1
- combine: bfloat16 [49152, 2], P(('expert', 'dp')), may hold values from 0.099609375 to 0.8984375
- w_in: bfloat16 [32, 2048, 1024], P('expert'), may hold values from -0.1875 to 0.1875
- w_out: bfloat16 [32, 2048, 1024], P('expert'), may hold values from -0.125 to 0.125
Outputs:
- grad_tokens: bfloat16 [49152, 1024], P(('expert', 'dp'))
- grad_combine: bfloat16 [49152, 2], P(('expert', 'dp'))
- grad_w_in: float32 [32, 2048, 1024], P('expert', 'dp')
- grad_w_out: float32 [32, 2048, 1024], P('expert', 'dp')
The draws below stay inside these ranges and needn't reach their ends.
Inputs may be any that keep to these rules, and one draw needn't show every extreme that they name: `routes`: each token names two different experts.
All inputs are finite; a program needn't handle non-finite values. No bound on the sum of `keep_second` on one device may be relied on, other than what follows from the above.
Results may differ from the reference program's by a relative error of at most 0.011.
Values may be sent and summed in bfloat16 or wider, within the bound.
A program may use at most 128 MiB of HBM per device.

```python
import jax
import jax.numpy as jnp
from jax import lax

D = 1024
FF = 2048
TOK_DEV = 192
EXPERTS = 32
TOKENS = 49152
CAP = 15
N_EXPERT = 32
N_DP = 8


def place_ends(drawn, own_key, smallest, largest):
    extent = drawn.shape
    spot = [jax.random.randint(jax.random.fold_in(own_key, axis), (), 0, extent[axis]) for axis in range(len(extent))]
    drawn = drawn.at[tuple(spot)].set(smallest)
    longest = extent.index(max(extent))
    spot[longest] = (spot[longest] + 1) % extent[longest]
    return drawn.at[tuple(spot)].set(largest)


def block_scale(rng, extent, cuts, smallest, top_value):
    def one(dim, parts):
        draws = jax.random.uniform(jax.random.fold_in(jax.random.fold_in(rng, 6), dim), (parts,), jnp.float32, smallest / len(cuts), top_value / len(cuts))
        return jnp.repeat(jnp.exp(draws), extent[dim] // parts).reshape((-1,) + (1,) * (len(extent) - dim - 1))

    gain = one(*cuts[0])
    for cut in cuts[1:]:
        gain = gain * one(*cut)
    return gain


def distinct(key, rows, number_of, top, lift):
    sequence = jax.random.permutation(jax.random.fold_in(key, 1), number_of)
    pull = sequence
    for power in range(3):
        pull = pull * pull // number_of
    pull = pull * lift // number_of
    tickets = jax.random.randint(jax.random.fold_in(key, 2), (rows, number_of), 0, 4096) + pull
    holders = jax.random.permutation(jax.random.fold_in(key, 3), rows)[jnp.arange(number_of) % rows]
    tickets = jnp.where(jnp.arange(rows)[:, None] == holders[None, :], 1 << 14, tickets)
    score = tickets * number_of + jnp.arange(number_of)
    return lax.top_k(score.astype(jnp.int32), top)[1].astype(jnp.int32)


def normal_values(own_key, extent, deviation, most, shards=(), kind=jnp.bfloat16):
    gain = block_scale(own_key, extent, shards, -0.22, 0.18) if shards else 1.0
    entries = jax.random.normal(own_key, extent, jnp.float32) * deviation * gain
    return jnp.minimum(jnp.maximum(entries, -most), most).astype(kind)


def setup_inputs(seed: int = 0) -> dict:
    streams_of = jax.random.split(jax.random.key(seed), 8)
    return {
        "tokens": normal_values(streams_of[0], (TOKENS, D), 1.0, 6.0, ((0, 256),)),
        "grad_out": normal_values(streams_of[1], (TOKENS, D), 1.0, 6.0, ((0, 256),)),
        "routes": distinct(streams_of[2], TOKENS, EXPERTS, 2, 1024),
        "keep_second": place_ends((jax.random.randint(streams_of[3], (TOKENS,), 0, 4) < 3).astype(jnp.int32), jax.random.fold_in(streams_of[3], 1), 0, 1),
        "combine": jnp.clip(0.099609375 + 0.7988281 * jax.random.uniform(streams_of[4], (TOKENS, 2), jnp.float32) ** block_scale(streams_of[4], (TOKENS, 2), ((0, 256),), -0.2, 0.2), 0.099609375, 0.8984375).astype(jnp.bfloat16),
        "w_in": normal_values(streams_of[5], (EXPERTS, FF, D), D ** -0.5, 0.1875, ((0, 32),)),
        "w_out": normal_values(streams_of[6], (EXPERTS, FF, D), FF ** -0.5, 0.125, ((0, 32),)),
    }


root_coef = 0.7978845608
cube_coef = 0.044715


def gelu_slope(hidden):
    inner_arg = root_coef * (hidden + cube_coef * hidden * hidden * hidden)
    tanh_val = jnp.tanh(inner_arg)
    active = 0.5 * hidden * (1.0 + tanh_val)
    derivative = 0.5 * (1.0 + tanh_val) + 0.5 * hidden * (1.0 - tanh_val * tanh_val) * root_coef * (1.0 + 3.0 * cube_coef * hidden * hidden)
    return active, derivative


def slot_index(routes, keep_second, expert_count, capacity):
    expert_ids = jnp.arange(expert_count, dtype=jnp.int32)
    first_hot = (routes[:, 0:1] == expert_ids[None, :]).astype(jnp.int32)
    second_hot = (routes[:, 1:2] == expert_ids[None, :]).astype(jnp.int32) * keep_second[:, None]
    first_pos = jnp.cumsum(first_hot, axis=0).astype(jnp.int32) - first_hot
    second_pos = jnp.cumsum(second_hot, axis=0).astype(jnp.int32) - second_hot + jnp.sum(first_hot, axis=0).astype(jnp.int32)[None, :]
    first_slot = jnp.sum(first_pos * first_hot, axis=1).astype(jnp.int32)
    second_slot = jnp.sum(second_pos * second_hot, axis=1).astype(jnp.int32)
    first_flat = jnp.where(first_slot < capacity, routes[:, 0] * capacity + first_slot, -1).astype(jnp.int32)
    second_live = (keep_second > 0) & (second_slot < capacity)
    second_flat = jnp.where(second_live, routes[:, 1] * capacity + second_slot, -1).astype(jnp.int32)
    slot_ids = jnp.arange(expert_count * capacity, dtype=jnp.int32)
    first_pick = slot_ids[:, None] == first_flat[None, :]
    second_pick = slot_ids[:, None] == second_flat[None, :]
    return first_pick, second_pick


def dispatch(tokens, grad_out, combine, first_pick, second_pick):
    chosen = (first_pick | second_pick).astype(jnp.bfloat16)
    sent_x = jnp.dot(chosen, tokens, preferred_element_type=jnp.float32).astype(jnp.bfloat16)
    sent_dy = jnp.dot(chosen, grad_out, preferred_element_type=jnp.float32).astype(jnp.bfloat16)
    weights = combine.astype(jnp.float32)
    sent_c = jnp.sum(jnp.where(first_pick, weights[None, :, 0], 0.0) + jnp.where(second_pick, weights[None, :, 1], 0.0), axis=1).astype(jnp.bfloat16)
    return sent_x, sent_dy, sent_c


def expert_rows(rows_x, rows_dy, rows_c, weight_in, weight_out):
    hidden = lax.dot_general(rows_x, weight_in, (((1,), (1,)), ((), ())), preferred_element_type=jnp.float32)
    active, derivative = gelu_slope(hidden)
    active_b = active.astype(jnp.bfloat16)
    output = jnp.dot(active_b, weight_out, preferred_element_type=jnp.float32)
    gate_grad = jnp.sum(output * rows_dy.astype(jnp.float32), axis=1).astype(jnp.bfloat16)
    scaled = (rows_c.astype(jnp.float32)[:, None] * rows_dy.astype(jnp.float32)).astype(jnp.bfloat16)
    active_grad = lax.dot_general(scaled, weight_out, (((1,), (1,)), ((), ())), preferred_element_type=jnp.float32)
    hidden_grad = (active_grad * derivative).astype(jnp.bfloat16)
    token_grad = jnp.dot(hidden_grad, weight_in, preferred_element_type=jnp.float32).astype(jnp.bfloat16)
    return token_grad, gate_grad, hidden_grad, active_b, scaled


def collect(token_back, gate_back, first_pick, second_pick):
    chosen = (first_pick | second_pick).astype(jnp.bfloat16)
    grad_tokens = lax.dot_general(chosen, token_back, (((0,), (0,)), ((), ())), preferred_element_type=jnp.float32).astype(jnp.bfloat16)
    gate_float = gate_back.astype(jnp.float32)[:, None]
    first_grad = jnp.sum(jnp.where(first_pick, gate_float, 0.0), axis=0)
    second_grad = jnp.sum(jnp.where(second_pick, gate_float, 0.0), axis=0)
    grad_combine = jnp.stack([first_grad, second_grad], axis=1).astype(jnp.bfloat16)
    return grad_tokens, grad_combine


def expert_full(bundle):
    rows_x, rows_dy, rows_c, weight_in, weight_out = bundle
    token_grad, gate_grad, hidden_grad, active_b, scaled = expert_rows(rows_x, rows_dy, rows_c, weight_in, weight_out)
    grad_in = lax.dot_general(hidden_grad, rows_x, (((0,), (0,)), ((), ())), preferred_element_type=jnp.float32)
    grad_outw = lax.dot_general(active_b, scaled, (((0,), (0,)), ((), ())), preferred_element_type=jnp.float32)
    return token_grad, gate_grad, grad_in, grad_outw


def regroup(array):
    shaped = array.reshape((N_EXPERT, N_DP, TOK_DEV) + array.shape[1:])
    return jnp.swapaxes(shaped, 0, 1)


def reference(tokens, grad_out, routes, keep_second, combine, w_in, w_out):
    capacity = CAP

    def one_group(totals, group_data):
        group_x, group_dy, group_routes, group_keep, group_combine = group_data
        first_pick, second_pick = jax.vmap(slot_index, in_axes=(0, 0, None, None))(group_routes, group_keep, EXPERTS, capacity)
        sent_x, sent_dy, sent_c = jax.vmap(dispatch)(group_x, group_dy, group_combine, first_pick, second_pick)
        rows_x = jnp.swapaxes(sent_x.reshape(N_EXPERT, EXPERTS, capacity, D), 0, 1).reshape(EXPERTS, N_EXPERT * capacity, D)
        rows_dy = jnp.swapaxes(sent_dy.reshape(N_EXPERT, EXPERTS, capacity, D), 0, 1).reshape(EXPERTS, N_EXPERT * capacity, D)
        rows_c = jnp.swapaxes(sent_c.reshape(N_EXPERT, EXPERTS, capacity), 0, 1).reshape(EXPERTS, N_EXPERT * capacity)
        token_grad, gate_grad, grad_in, grad_outw = lax.map(expert_full, (rows_x, rows_dy, rows_c, w_in, w_out))
        token_back = jnp.swapaxes(token_grad.reshape(EXPERTS, N_EXPERT, capacity, D), 0, 1).reshape(N_EXPERT, EXPERTS * capacity, D)
        gate_back = jnp.swapaxes(gate_grad.reshape(EXPERTS, N_EXPERT, capacity), 0, 1).reshape(N_EXPERT, EXPERTS * capacity)
        grad_part, combine_part = jax.vmap(collect)(token_back, gate_back, first_pick, second_pick)
        return (totals[0] + grad_in, totals[1] + grad_outw), (grad_part, combine_part)

    zero_grad = jnp.zeros((EXPERTS, FF, D), jnp.float32)
    streams = (regroup(tokens), regroup(grad_out), regroup(routes), regroup(keep_second), regroup(combine))
    sums, pieces = lax.scan(one_group, (zero_grad, zero_grad), streams)
    grad_tokens = jnp.swapaxes(pieces[0], 0, 1).reshape(N_EXPERT * N_DP * TOK_DEV, D)
    grad_combine = jnp.swapaxes(pieces[1], 0, 1).reshape(N_EXPERT * N_DP * TOK_DEV, 2)
    return grad_tokens, grad_combine, sums[0], sums[1]
```

```python
import functools

import jax
import jax.numpy as jnp
from jax import lax
from jax.experimental import pallas as pl
from jax.experimental.pallas import tpu as pltpu
from jax.sharding import PartitionSpec as P

MESH = pl.DeviceIdType.MESH
F32, BF16 = jnp.float32, jnp.bfloat16
root_coef = 0.7978845608
cube_coef = 0.044715
SLOT = 16
GATE = 128


def dot(a, b, ca, cb):
    return lax.dot_general(a, b, (((ca,), (cb,)), ((), ())), preferred_element_type=F32)


def gelu_slope(hidden):
    square = hidden * hidden
    tanh_val = jnp.tanh(root_coef * (hidden + cube_coef * square * hidden))
    half = 0.5 * (1.0 + tanh_val)
    slope = half + 0.5 * hidden * (1.0 - tanh_val * tanh_val) * root_coef * (
        1.0 + 3.0 * cube_coef * square
    )
    return hidden * half, slope


def kernel(
    capacity, n_x, n_y,
    tok_hbm, dy_hbm, routes_ref, keep_ref, comb_ref, win_hbm, wout_hbm,
    gtok_ref, gcomb_ref, gin_ref, gout_ref,
    tok, dy, ptok, pdy, meta, pmeta, win, wout,
    sent_x, sent_s, psent_x, psent_s, own_x, own_s, part_x, part_s,
    first_m, second_m, hg_buf, act_buf, tg_acc, gate_acc, back_out, back_in,
    term, got,
    load_sem, pair_send, pair_recv,
    xs, xr, ss, sr, pxs, pxr, pss, psr, bs, br, ring_send, ring_recv,
):
    me = lax.axis_index("expert")
    z = lax.axis_index("dp")
    n_e = n_x * n_y * 2
    n_z = lax.axis_size("dp")
    toks, width = tok.shape
    rows = n_e * SLOT
    core, cx, cy = lax.rem(me, 2), lax.rem(me // 2, n_x), me // (2 * n_x)
    up, down = lax.rem(z + 1, n_z), lax.rem(z + n_z - 1, n_z)
    far = lax.rem(z + n_z // 2, n_z)

    def peer(q):
        cell = lax.rem(q, n_x * n_y)
        dx, dy_ = lax.rem(cell, n_x) + 1, cell // n_x + 1
        dc = 1 - q // (n_x * n_y)
        x, y, c = lax.rem(cx + dx, n_x), lax.rem(cy + dy_, n_y), lax.rem(core + dc, 2)
        return (y * n_x + x) * 2 + c

    loads = [
        pltpu.make_async_copy(src, dst, load_sem.at[k])
        for k, (src, dst) in enumerate(
            ((tok_hbm, tok), (dy_hbm, dy), (win_hbm.at[0], win), (wout_hbm.at[0], wout))
        )
    ]
    for c in loads:
        c.start()

    barrier = pltpu.get_barrier_semaphore()
    for other in (far, up, down):
        pl.semaphore_signal(barrier, inc=1, device_id=(me, other), device_id_type=MESH)

    def greet(q, carry):
        pl.semaphore_signal(barrier, inc=1, device_id=(peer(q), z), device_id_type=MESH)
        return carry

    lax.fori_loop(0, n_e - 1, greet, 0)

    expert_ids = lax.broadcasted_iota(jnp.int32, (n_e, toks), 0)
    r0, r1 = routes_ref[0:1, :], routes_ref[1:2, :]
    keep = keep_ref[...]
    first_hot = jnp.where(r0 == expert_ids, 1.0, 0.0)
    second_hot = jnp.where((r1 == expert_ids) & (keep > 0), 1.0, 0.0)
    earlier = jnp.where(
        lax.broadcasted_iota(jnp.int32, (toks, toks), 0)
        < lax.broadcasted_iota(jnp.int32, (toks, toks), 1), 1.0, 0.0,
    ).astype(BF16)
    first_pos = dot(first_hot.astype(BF16), earlier, 1, 0)
    second_pos = dot(second_hot.astype(BF16), earlier, 1, 0) + jnp.sum(
        first_hot, axis=1, keepdims=True
    )
    first_slot = jnp.sum(first_pos * first_hot, axis=0, keepdims=True)
    second_slot = jnp.sum(second_pos * second_hot, axis=0, keepdims=True)
    first_flat = jnp.where(first_slot < capacity, r0.astype(F32) * SLOT + first_slot, -1.0)
    second_flat = jnp.where(
        (keep > 0) & (second_slot < capacity), r1.astype(F32) * SLOT + second_slot, -1.0
    )
    weight = comb_ref[...].astype(F32)
    meta[0:1, :] = first_flat
    meta[1:2, :] = second_flat
    meta[2:4, :] = weight
    meta[4:8, :] = jnp.zeros((4, toks), F32)
    w0, w1 = weight[0:1, :], weight[1:2, :]
    slot_ids = lax.broadcasted_iota(jnp.int32, (rows, toks), 0).astype(F32)
    hit0, hit1 = slot_ids == first_flat, slot_ids == second_flat
    first_m[...] = jnp.where(hit0, 1.0, 0.0).astype(BF16)
    second_m[...] = jnp.where(hit1, 1.0, 0.0).astype(BF16)
    loads[0].wait()
    sent_x[...] = dot(first_m[...] + second_m[...], tok[...], 1, 0).astype(BF16).reshape(
        n_e, SLOT, width
    )
    weighted = jnp.where(hit0, w0, 0.0) + jnp.where(hit1, w1, 0.0)
    loads[1].wait()
    sent_s[...] = dot(weighted.astype(BF16), dy[...], 1, 0).astype(BF16).reshape(n_e, SLOT, width)

    pl.semaphore_wait(barrier, n_e + 2)

    pair = [
        pltpu.make_async_remote_copy(
            src_ref=src, dst_ref=dst, send_sem=pair_send.at[k], recv_sem=pair_recv.at[k],
            device_id=(me, far), device_id_type=MESH,
        )
        for k, (src, dst) in enumerate(((meta, pmeta), (tok, ptok), (dy, pdy)))
    ]
    for c in pair:
        c.start()

    def hop(src, dst, send, recv, other, slot):
        return pltpu.make_async_remote_copy(
            src_ref=src.at[other], dst_ref=dst.at[slot], send_sem=send.at[other],
            recv_sem=recv.at[slot], device_id=(other, z), device_id_type=MESH,
        )

    def spread(lanes):
        def body(q, carry):
            other = peer(q)
            for src, dst, send, recv in lanes:
                hop(src, dst, send, recv, other, me).start()
            return carry

        lax.fori_loop(0, n_e - 1, body, 0)

    def arrive(lanes):
        def body(q, carry):
            other = lax.rem(me + 1 + q, n_e)
            for src, dst, send, recv in lanes:
                hop(src, dst, send, recv, other, other).wait_recv()
            return carry

        lax.fori_loop(0, n_e - 1, body, 0)

    def drain(lanes):
        def body(q, carry):
            other = lax.rem(me + 1 + q, n_e)
            for src, dst, send, recv in lanes:
                hop(src, dst, send, recv, other, other).wait_send()
            return carry

        lax.fori_loop(0, n_e - 1, body, 0)

    lane_x, lane_s = (sent_x, own_x, xs, xr), (sent_s, own_s, ss, sr)
    lane_px, lane_ps = (psent_x, part_x, pxs, pxr), (psent_s, part_s, pss, psr)
    lane_b = (back_out, back_in, bs, br)
    spread((lane_x, lane_s))
    own_x[me] = sent_x[me]
    own_s[me] = sent_s[me]

    pair[0].wait_recv()
    pair[1].wait_recv()
    p0, p1 = pmeta[0:1, :], pmeta[1:2, :]
    q0, q1 = pmeta[2:3, :], pmeta[3:4, :]
    chosen = jnp.where((slot_ids == p0) | (slot_ids == p1), 1.0, 0.0).astype(BF16)
    psent_x[...] = dot(chosen, ptok[...], 1, 0).astype(BF16).reshape(n_e, SLOT, width)
    spread((lane_px,))
    part_x[me] = psent_x[me]

    half = 128
    ff_dev = gin_ref.shape[0]
    chunks = win.shape[0] // ff_dev
    loads[2].wait()
    loads[3].wait()
    arrive((lane_x, lane_s))
    tg_acc[...] = jnp.zeros_like(tg_acc)
    gate_acc[...] = jnp.zeros_like(gate_acc)

    def own_chunk(c, carry):
        cut = pl.ds(pl.multiple_of(c * ff_dev, ff_dev), ff_dev)
        block = rows // 2
        src = n_e // 2
        for r in range(2):
            x_r = own_x[r * src:(r + 1) * src].reshape(block, width)
            s_r = own_s[r * src:(r + 1) * src].reshape(block, width)
            active, slope = gelu_slope(dot(x_r, win[cut, :], 1, 1))
            active_grad = dot(s_r, wout[cut, :], 1, 1)
            active = active.astype(BF16)
            hidden_grad = (active_grad * slope).astype(BF16)
            piece = pl.ds(r * block, block)
            for k in range(ff_dev // half):
                at = c * (ff_dev // half) + k
                act_buf[at, piece, :] = active[:, k * half:(k + 1) * half]
                hg_buf[at, piece, :] = hidden_grad[:, k * half:(k + 1) * half]
            product = active.astype(F32) * active_grad
            gate_acc[piece, :] += product[:, :half] + product[:, half:]
            tg_acc[piece, :] += dot(hidden_grad, win[cut, :], 1, 0)
        return carry

    lax.fori_loop(0, chunks // 2, own_chunk, 0)

    pair[2].wait_recv()
    weighted = jnp.where(slot_ids == p0, q0, 0.0) + jnp.where(slot_ids == p1, q1, 0.0)
    psent_s[...] = dot(weighted.astype(BF16), pdy[...], 1, 0).astype(BF16).reshape(
        n_e, SLOT, width
    )
    spread((lane_ps,))
    part_s[me] = psent_s[me]

    lax.fori_loop(chunks // 2, chunks, own_chunk, 0)
    back_out[:, :, :width] = tg_acc[...].astype(BF16).reshape(n_e, SLOT, width)
    gate = jnp.sum(gate_acc[...], axis=1, keepdims=True)
    back_out[:, :, width:] = jnp.broadcast_to(gate, (rows, GATE)).astype(BF16).reshape(
        n_e, SLOT, GATE
    )
    spread((lane_b,))
    back_in[me] = back_out[me]

    arrive((lane_px, lane_ps))

    def near(at, store):
        cut = pl.ds(pl.multiple_of(at * half, half), half)
        x_p, s_p = part_x[...].reshape(rows, width), part_s[...].reshape(rows, width)
        active, slope = gelu_slope(dot(x_p, win[cut, :], 1, 1))
        hidden_grad = (dot(s_p, wout[cut, :], 1, 1) * slope).astype(BF16)
        active = active.astype(BF16)
        x_o, s_o = own_x[...].reshape(rows, width), own_s[...].reshape(rows, width)
        store(
            dot(hg_buf[at], x_o, 0, 0) + dot(hidden_grad, x_p, 0, 0),
            dot(act_buf[at], s_o, 0, 0) + dot(active, s_p, 0, 0),
        )

    def ring(k, other):
        return pltpu.make_async_remote_copy(
            src_ref=term.at[k], dst_ref=got.at[k], send_sem=ring_send.at[k],
            recv_sem=ring_recv.at[k], device_id=(me, other), device_id_type=MESH,
        )

    def to_term(k):
        def store(a, b):
            term[k, :, :width] = a.astype(BF16)
            term[k, :, width:] = b.astype(BF16)

        return store

    targets = (
        2 * lax.rem(z + 2, n_z), 2 * lax.rem(z + n_z - 2, n_z) + 1,
        2 * up + 1, 2 * down, 2 * up, 2 * down + 1,
    )
    for k in range(4):
        near(targets[k], to_term(k))
        ring(k, up if k % 2 == 0 else down).start()
    for k in range(4, 6):
        near(targets[k], to_term(k))

    for k in range(2):
        def to_out(a, b, k=k):
            gin_ref[k * half:(k + 1) * half, :] = a
            gout_ref[k * half:(k + 1) * half, :] = b

        near(2 * z + k, to_out)

    for k in range(2):
        ring(k, up if k % 2 == 0 else down).wait_recv()
        term[4 + k] = (term[4 + k].astype(F32) + got[k].astype(F32)).astype(BF16)
        ring(4 + k, up if k % 2 == 0 else down).start()

    arrive((lane_b,))
    back = back_in[...].reshape(rows, width + GATE)
    gtok_ref[...] = dot(first_m[...] + second_m[...], back[:, :width], 0, 0).astype(BF16)
    for k, hits in enumerate((first_m, second_m)):
        grad = dot(back[:, width:], hits[...], 0, 0)
        gcomb_ref[k:k + 1, :] = (grad[0:1, :] / meta[2 + k:3 + k, :]).astype(BF16)

    def gather(k, part):
        piece = slice(part * half, (part + 1) * half)
        gin_ref[piece, :] += got[k, :, :width].astype(F32)
        gout_ref[piece, :] += got[k, :, width:].astype(F32)

    for k, part in ((2, 1), (3, 0), (4, 0), (5, 1)):
        ring(k, up if k % 2 == 0 else down).wait_recv()
        gather(k, part)

    for c in pair:
        c.wait_send()
    drain((lane_x, lane_s, lane_px, lane_ps, lane_b))
    for k in range(6):
        ring(k, up if k % 2 == 0 else down).wait_send()


def per_device(n_x, n_y, tokens, grad_out, routes, keep_second, combine, w_in, w_out):
    n_e = lax.axis_size("expert")
    toks, width = tokens.shape
    ff = w_in.shape[1]
    ff_dev = ff // lax.axis_size("dp")
    capacity = 5 * toks // (2 * n_e)
    rows = n_e * SLOT
    half = 128
    any_spec = pl.BlockSpec(memory_space=pl.ANY)
    vmem_spec = pl.BlockSpec(memory_space=pltpu.VMEM)
    slots = pltpu.VMEM((n_e, SLOT, width), BF16)
    sems = pltpu.SemaphoreType.DMA((n_e,))
    gtok, gcomb, gin, gout = pl.pallas_call(
        functools.partial(kernel, capacity, n_x, n_y),
        out_shape=(
            jax.ShapeDtypeStruct((toks, width), BF16),
            jax.ShapeDtypeStruct((2, toks), BF16),
            jax.ShapeDtypeStruct((ff_dev, width), F32),
            jax.ShapeDtypeStruct((ff_dev, width), F32),
        ),
        in_specs=[any_spec, any_spec, vmem_spec, vmem_spec, vmem_spec, any_spec, any_spec],
        out_specs=(vmem_spec,) * 4,
        scratch_shapes=[pltpu.VMEM((toks, width), BF16)] * 4
        + [pltpu.VMEM((8, toks), F32)] * 2
        + [pltpu.VMEM((ff, width), BF16)] * 2
        + [slots] * 8
        + [pltpu.VMEM((rows, toks), BF16)] * 2
        + [pltpu.VMEM((ff // half, rows, half), BF16)] * 2
        + [pltpu.VMEM((rows, width), F32), pltpu.VMEM((rows, half), F32)]
        + [pltpu.VMEM((n_e, SLOT, width + GATE), BF16)] * 2
        + [pltpu.VMEM((6, half, 2 * width), BF16)] * 2
        + [pltpu.SemaphoreType.DMA((4,)), pltpu.SemaphoreType.DMA((3,)), pltpu.SemaphoreType.DMA((3,))]
        + [sems] * 10
        + [pltpu.SemaphoreType.DMA((6,))] * 2,
        compiler_params=pltpu.CompilerParams(
            collective_id=0, has_side_effects=True, vmem_limit_bytes=60 * 2**20
        ),
    )(
        tokens, grad_out, routes.T, keep_second.reshape(1, toks), combine.T, w_in, w_out,
    )
    return gtok, gcomb.T, gin[None], gout[None]


def solution(mesh):
    n_e = mesh.shape["expert"]
    n_x = 4
    return jax.shard_map(
        functools.partial(per_device, n_x, n_e // (2 * n_x)),
        mesh=mesh,
        in_specs=(
            P(("expert", "dp"), None),
            P(("expert", "dp"), None),
            P(("expert", "dp"), None),
            P(("expert", "dp")),
            P(("expert", "dp"), None),
            P("expert", None, None),
            P("expert", None, None),
        ),
        out_specs=(
            P(("expert", "dp"), None),
            P(("expert", "dp"), None),
            P("expert", "dp", None),
            P("expert", "dp", None),
        ),
        check_vma=False,
    )
```

```python
import functools

import jax
import jax.numpy as jnp
from jax import lax
from jax.experimental import pallas as pl
from jax.experimental.pallas import tpu as pltpu
from jax.sharding import PartitionSpec as P

MESH = pl.DeviceIdType.MESH
F32, BF16 = jnp.float32, jnp.bfloat16
root_coef = 0.7978845608
cube_coef = 0.044715
SLOT = 16
GATE = 128
LONG = 64


def dot(a, b, ca, cb):
    return lax.dot_general(a, b, (((ca,), (cb,)), ((), ())), preferred_element_type=F32)


def gelu_slope(hidden):
    square = hidden * hidden
    tanh_val = jnp.tanh(root_coef * (hidden + cube_coef * square * hidden))
    half = 0.5 * (1.0 + tanh_val)
    slope = half + 0.5 * hidden * (1.0 - tanh_val * tanh_val) * root_coef * (
        1.0 + 3.0 * cube_coef * square
    )
    return hidden * half, slope


def kernel(
    capacity, n_x, n_y,
    tok_hbm, dy_hbm, routes_ref, keep_ref, comb_ref, win_hbm, wout_hbm,
    gtok_ref, gcomb_ref, gin_ref, gout_ref,
    tok, dy, ptok, pdy, meta, pmeta, win, wout,
    sent, psent_x, psent_s, own, part_x, part_s,
    first_m, second_m, hg_buf, act_buf, tg_acc, gate_acc, back_out, back_in,
    far_term, far_got, term, got,
    load_sem, pair_send, pair_recv,
    lane_send, lane_recv, ring_send, ring_recv, far_send, far_recv,
):
    me = lax.axis_index("expert")
    z = lax.axis_index("dp")
    n_e = n_x * n_y * 2
    n_z = lax.axis_size("dp")
    toks, width = tok.shape
    rows = n_e * SLOT
    core, cx, cy = lax.rem(me, 2), lax.rem(me // 2, n_x), me // (2 * n_x)
    up, down = lax.rem(z + 1, n_z), lax.rem(z + n_z - 1, n_z)
    far = lax.rem(z + n_z // 2, n_z)

    def peer(q):
        cell = lax.rem(q, n_x * n_y)
        dx, dy_ = lax.rem(cell, n_x) + 1, cell // n_x + 1
        dc = 1 - q // (n_x * n_y)
        x, y, c = lax.rem(cx + dx, n_x), lax.rem(cy + dy_, n_y), lax.rem(core + dc, 2)
        return (y * n_x + x) * 2 + c

    barrier = pltpu.get_barrier_semaphore()
    for other in (far, up, down):
        pl.semaphore_signal(barrier, inc=1, device_id=(me, other), device_id_type=MESH)

    ahead_x = [lax.rem(cx + k, n_x) * 2 for k in range(n_x)]
    ahead_y = [lax.rem(cy + k, n_y) * (2 * n_x) for k in range(n_y)]
    cells = sorted(
        ((dx, dy_) for dx in range(n_x) for dy_ in range(n_y)),
        key=lambda cell: -min(cell[0], n_x - cell[0]) - min(cell[1], n_y - cell[1]),
    )
    for dx, dy_ in cells:
        for c in (core, 1 - core)[0 if dx + dy_ else 1:]:
            pl.semaphore_signal(
                barrier, inc=1, device_id=(ahead_y[dy_] + ahead_x[dx] + c, z), device_id_type=MESH
            )

    loads = [
        pltpu.make_async_copy(src, dst, load_sem.at[k])
        for k, (src, dst) in enumerate(
            ((tok_hbm, tok), (dy_hbm, dy), (win_hbm.at[0], win), (wout_hbm.at[0], wout))
        )
    ]
    for c in loads:
        c.start()

    expert_ids = lax.broadcasted_iota(jnp.int32, (n_e, toks), 0)
    r0, r1 = routes_ref[0:1, :], routes_ref[1:2, :]
    keep = keep_ref[...]
    first_hot = jnp.where(r0 == expert_ids, 1.0, 0.0)
    second_hot = jnp.where((r1 == expert_ids) & (keep > 0), 1.0, 0.0)
    earlier = jnp.where(
        lax.broadcasted_iota(jnp.int32, (toks, toks), 0)
        < lax.broadcasted_iota(jnp.int32, (toks, toks), 1), 1.0, 0.0,
    ).astype(BF16)
    first_pos = dot(first_hot.astype(BF16), earlier, 1, 0)
    second_pos = dot(second_hot.astype(BF16), earlier, 1, 0) + jnp.sum(
        first_hot, axis=1, keepdims=True
    )
    first_slot = jnp.sum(first_pos * first_hot, axis=0, keepdims=True)
    second_slot = jnp.sum(second_pos * second_hot, axis=0, keepdims=True)
    first_flat = jnp.where(first_slot < capacity, r0.astype(F32) * SLOT + first_slot, -1.0)
    second_flat = jnp.where(
        (keep > 0) & (second_slot < capacity), r1.astype(F32) * SLOT + second_slot, -1.0
    )
    weight = comb_ref[...].astype(F32)
    meta[0:1, :] = first_flat
    meta[1:2, :] = second_flat
    meta[2:4, :] = weight
    meta[4:8, :] = jnp.zeros((4, toks), F32)
    w0, w1 = weight[0:1, :], weight[1:2, :]
    slot_ids = lax.broadcasted_iota(jnp.int32, (rows, toks), 0).astype(F32)
    hit0, hit1 = slot_ids == first_flat, slot_ids == second_flat
    first_m[...] = jnp.where(hit0, 1.0, 0.0).astype(BF16)
    second_m[...] = jnp.where(hit1, 1.0, 0.0).astype(BF16)
    loads[0].wait()
    sent[:, 0] = dot(first_m[...] + second_m[...], tok[...], 1, 0).astype(BF16).reshape(
        n_e, SLOT, width
    )
    weighted = jnp.where(hit0, w0, 0.0) + jnp.where(hit1, w1, 0.0)
    loads[1].wait()
    sent[:, 1] = dot(weighted.astype(BF16), dy[...], 1, 0).astype(BF16).reshape(n_e, SLOT, width)

    pl.semaphore_wait(barrier, n_e + 2)

    pair = [
        pltpu.make_async_remote_copy(
            src_ref=src, dst_ref=dst, send_sem=pair_send.at[k], recv_sem=pair_recv.at[k],
            device_id=(me, far), device_id_type=MESH,
        )
        for k, (src, dst) in enumerate(((meta, pmeta), (tok, ptok), (dy, pdy)))
    ]
    for c in pair:
        c.start()

    lanes = ((sent, own), (psent_x, part_x), (psent_s, part_s), (back_out, back_in))

    def hop(lane, src, dst, other):
        return pltpu.make_async_remote_copy(
            src_ref=lanes[lane][0].at[src], dst_ref=lanes[lane][1].at[dst],
            send_sem=lane_send.at[lane], recv_sem=lane_recv.at[lane],
            device_id=(other, z), device_id_type=MESH,
        )

    def spread(lane):
        def body(q, carry):
            other = peer(q)
            hop(lane, other, me, other).start()
            return carry

        lax.fori_loop(0, n_e - 1, body, 0)
        lanes[lane][1][me] = lanes[lane][0][me]

    def whole(lane):
        return hop(lane, pl.ds(0, n_e - 1), pl.ds(0, n_e - 1), lax.rem(me + 1, n_e))

    spread(0)

    pair[0].wait_recv()
    pair[1].wait_recv()
    p0, p1 = pmeta[0:1, :], pmeta[1:2, :]
    q0, q1 = pmeta[2:3, :], pmeta[3:4, :]
    chosen = jnp.where((slot_ids == p0) | (slot_ids == p1), 1.0, 0.0).astype(BF16)
    psent_x[...] = dot(chosen, ptok[...], 1, 0).astype(BF16).reshape(n_e, SLOT, width)
    spread(1)

    ff_dev = gin_ref.shape[0]
    near_rows = ff_dev - LONG
    chunks = win.shape[0] // ff_dev
    loads[2].wait()
    loads[3].wait()
    whole(0).wait_recv()
    tg_acc[...] = jnp.zeros_like(tg_acc)
    gate_acc[...] = jnp.zeros_like(gate_acc)
    block, src = rows // 2, n_e // 2

    def own_chunk(j, carry):
        odd = lax.rem(j, 2)
        target = lax.rem(z + n_z // 2 + (1 - odd) * (j // 2) - odd * ((j + 1) // 2), n_z)
        cut = pl.ds(pl.multiple_of(target * ff_dev, ff_dev), ff_dev)
        for r in range(2):
            x_r = own[r * src:(r + 1) * src, 0].reshape(block, width)
            s_r = own[r * src:(r + 1) * src, 1].reshape(block, width)
            active, slope = gelu_slope(dot(x_r, win[cut, :], 1, 1))
            active_grad = dot(s_r, wout[cut, :], 1, 1)
            active = active.astype(BF16)
            hidden_grad = (active_grad * slope).astype(BF16)
            piece = pl.ds(r * block, block)
            act_buf[target, piece, :] = active
            hg_buf[target, piece, :] = hidden_grad
            product = active.astype(F32) * active_grad
            gate_acc[piece, :] += product[:, :GATE] + product[:, GATE:]
            tg_acc[piece, :] += dot(hidden_grad, win[cut, :], 1, 0)
        for m, left in enumerate((hg_buf, act_buf)):
            part = dot(
                left[target, :, ff_dev - 128:], own[:, m].reshape(rows, width), 0, 0
            )
            far_term[j, m] = part[128 - LONG:].astype(BF16)
        return carry

    def own_chunks(start, stop):
        lax.fori_loop(start, stop, own_chunk, 0)

    long_up = ((0, 0), (1, 1), (1, 0), (3, 1), (3, 0), (5, 1), (5, 0))
    long_down = ((0, 1), (2, 0), (2, 1), (4, 0), (4, 1), (6, 0), (6, 1))

    def long_hop(side, k):
        j, m = (long_up, long_down)[side][k]
        return pltpu.make_async_remote_copy(
            src_ref=far_term.at[j, m], dst_ref=far_got.at[side, k],
            send_sem=far_send.at[side, k], recv_sem=far_recv.at[side, k],
            device_id=(me, (up, down)[side]), device_id_type=MESH,
        )

    def relay(k):
        for side in range(2):
            j, m = (long_up, long_down)[side][k + 2]
            long_hop(side, k).wait_recv()
            far_term[j, m] = (far_term[j, m].astype(F32) + far_got[side, k].astype(F32)).astype(BF16)
            long_hop(side, k + 2).start()

    own_chunks(0, 3)
    for k in range(2):
        for side in range(2):
            long_hop(side, k).start()
    own_chunks(3, 4)

    pair[2].wait_recv()
    weighted = jnp.where(slot_ids == p0, q0, 0.0) + jnp.where(slot_ids == p1, q1, 0.0)
    psent_s[...] = dot(weighted.astype(BF16), pdy[...], 1, 0).astype(BF16).reshape(
        n_e, SLOT, width
    )
    spread(2)

    own_chunks(4, 5)
    relay(0)
    own_chunks(5, 6)
    relay(1)
    own_chunks(6, 8)
    relay(2)
    back_out[:, :, :width] = tg_acc[...].astype(BF16).reshape(n_e, SLOT, width)
    gate = jnp.sum(gate_acc[...], axis=1, keepdims=True)
    back_out[:, :, width:] = jnp.broadcast_to(gate, (rows, GATE)).astype(BF16).reshape(
        n_e, SLOT, GATE
    )
    relay(3)
    whole(1).wait_recv()
    whole(2).wait_recv()
    def near(target, store_in, store_out):
        cut = pl.ds(pl.multiple_of(target * ff_dev, ff_dev), ff_dev)
        x_p, s_p = part_x[...].reshape(rows, width), part_s[...].reshape(rows, width)
        x_o, s_o = own[:, 0].reshape(rows, width), own[:, 1].reshape(rows, width)
        active, slope = gelu_slope(dot(x_p, win[cut, :], 1, 1))
        if store_in:
            hidden_grad = (dot(s_p, wout[cut, :], 1, 1) * slope).astype(BF16)
            grad = dot(hg_buf[target], x_o, 0, 0) + dot(hidden_grad, x_p, 0, 0)
            store_in(grad[:near_rows])
        if store_out:
            grad = dot(act_buf[target], s_o, 0, 0) + dot(active.astype(BF16), s_p, 0, 0)
            store_out(grad[:near_rows])

    def ring(k):
        return pltpu.make_async_remote_copy(
            src_ref=term.at[k], dst_ref=got.at[k], send_sem=ring_send.at[k],
            recv_sem=ring_recv.at[k], device_id=(me, down if k % 2 else up), device_id_type=MESH,
        )

    def to_term(k):
        def store(grad):
            term[k] = grad.astype(BF16)

        return store

    def to_out(ref):
        def store(grad):
            ref[:near_rows, :] = grad

        return store

    near(lax.rem(z + 2, n_z), to_term(0), None)
    ring(0).start()
    near(lax.rem(z + n_z - 2, n_z), None, to_term(1))
    ring(1).start()
    relay(4)
    spread(3)
    near(up, to_term(4), to_term(2))
    ring(2).start()
    near(down, to_term(3), to_term(5))
    ring(3).start()
    near(z, to_out(gin_ref), to_out(gout_ref))
    for m, (ref, k_up, k_down) in enumerate(((gin_ref, 6, 5), (gout_ref, 5, 6))):
        long_hop(0, k_up).wait_recv()
        long_hop(1, k_down).wait_recv()
        ref[near_rows:, :] = (
            far_term[chunks - 1, m].astype(F32)
            + far_got[0, k_up].astype(F32) + far_got[1, k_down].astype(F32)
        )
    for k in range(2):
        ring(k).wait_recv()
        term[4 + k] = (term[4 + k].astype(F32) + got[k].astype(F32)).astype(BF16)
        ring(4 + k).start()

    whole(3).wait_recv()
    back = back_in[...].reshape(rows, width + GATE)
    gtok_ref[...] = dot(first_m[...] + second_m[...], back[:, :width], 0, 0).astype(BF16)
    for k, hits in enumerate((first_m, second_m)):
        grad = dot(back[:, width:], hits[...], 0, 0)
        gcomb_ref[k:k + 1, :] = (grad[0:1, :] / meta[2 + k:3 + k, :]).astype(BF16)

    for k, ref in ((2, gout_ref), (3, gin_ref), (4, gin_ref), (5, gout_ref)):
        ring(k).wait_recv()
        ref[:near_rows, :] += got[k].astype(F32)

    for c in pair:
        c.wait_send()
    for lane in range(len(lanes)):
        whole(lane).wait_send()
    for k in range(6):
        ring(k).wait_send()
    for side in range(2):
        for k in range(len(long_up)):
            long_hop(side, k).wait_send()


def hand_out(*refs):
    copies = [pltpu.make_async_copy(refs[k], refs[4 + k], refs[8].at[k]) for k in range(4)]
    for c in copies:
        c.start()
    for c in copies:
        c.wait()


def per_device(n_x, n_y, tokens, grad_out, routes, keep_second, combine, w_in, w_out):
    n_e = lax.axis_size("expert")
    toks, width = tokens.shape
    ff = w_in.shape[1]
    ff_dev = ff // lax.axis_size("dp")
    capacity = 5 * toks // (2 * n_e)
    rows = n_e * SLOT
    any_spec = pl.BlockSpec(memory_space=pltpu.HBM)
    vmem_spec = pl.BlockSpec(memory_space=pltpu.VMEM)
    slots = pltpu.VMEM((n_e, SLOT, width), BF16)
    pairs = pltpu.VMEM((n_e, 2, SLOT, width), BF16)
    results = pl.pallas_call(
        functools.partial(kernel, capacity, n_x, n_y),
        out_shape=(
            pltpu.VMEM((toks, width), BF16),
            pltpu.VMEM((2, toks), BF16),
            pltpu.VMEM((ff_dev, width), F32),
            pltpu.VMEM((ff_dev, width), F32),
        ),
        in_specs=[any_spec, any_spec, vmem_spec, vmem_spec, vmem_spec, any_spec, any_spec],
        out_specs=(vmem_spec,) * 4,
        scratch_shapes=[pltpu.VMEM((toks, width), BF16)] * 4
        + [pltpu.VMEM((8, toks), F32)] * 2
        + [pltpu.VMEM((ff, width), BF16)] * 2
        + [pairs, slots, slots, pairs, slots, slots]
        + [pltpu.VMEM((rows, toks), BF16)] * 2
        + [pltpu.VMEM((ff // ff_dev, rows, ff_dev), BF16)] * 2
        + [pltpu.VMEM((rows, width), F32), pltpu.VMEM((rows, GATE), F32)]
        + [pltpu.VMEM((n_e, SLOT, width + GATE), BF16)] * 2
        + [pltpu.VMEM((ff // ff_dev, 2, LONG, width), BF16), pltpu.VMEM((2, 7, LONG, width), BF16)]
        + [pltpu.VMEM((6, ff_dev - LONG, width), BF16)] * 2
        + [pltpu.SemaphoreType.DMA((4,)), pltpu.SemaphoreType.DMA((3,)), pltpu.SemaphoreType.DMA((3,))]
        + [pltpu.SemaphoreType.DMA((4,))] * 2
        + [pltpu.SemaphoreType.DMA((6,))] * 2
        + [pltpu.SemaphoreType.DMA((2, 7))] * 2,
        compiler_params=pltpu.CompilerParams(
            collective_id=0, has_side_effects=True, vmem_limit_bytes=58 * 2**20
        ),
    )(
        tokens, grad_out, routes.T, keep_second.reshape(1, toks), combine.T, w_in, w_out,
    )
    gtok, gcomb, gin, gout = pl.pallas_call(
        hand_out,
        out_shape=tuple(jax.ShapeDtypeStruct(r.shape, r.dtype) for r in results),
        in_specs=[vmem_spec] * 4,
        out_specs=(any_spec,) * 4,
        scratch_shapes=[pltpu.SemaphoreType.DMA((4,))],
        compiler_params=pltpu.CompilerParams(vmem_limit_bytes=8 * 2**20),
    )(*results)
    return gtok, gcomb.T, gin[None], gout[None]


def solution(mesh):
    n_e = mesh.shape["expert"]
    n_x = 4
    return jax.shard_map(
        functools.partial(per_device, n_x, n_e // (2 * n_x)),
        mesh=mesh,
        in_specs=(
            P(("expert", "dp"), None),
            P(("expert", "dp"), None),
            P(("expert", "dp"), None),
            P(("expert", "dp")),
            P(("expert", "dp"), None),
            P("expert", None, None),
            P("expert", None, None),
        ),
        out_specs=(
            P(("expert", "dp"), None),
            P(("expert", "dp"), None),
            P("expert", "dp", None),
            P("expert", "dp", None),
        ),
        check_vma=False,
    )
```

```python
import functools

import jax
import jax.numpy as jnp
from jax import lax
from jax.experimental import pallas as pl
from jax.experimental.pallas import tpu as pltpu
from jax.sharding import PartitionSpec as P

MESH = pl.DeviceIdType.MESH
F32, BF16 = jnp.float32, jnp.bfloat16
root_coef = 0.7978845608
cube_coef = 0.044715
SLOT = 16
GATE = 128
PARTS = 2
LONG = 48


def dot(a, b, ca, cb):
    return lax.dot_general(a, b, (((ca,), (cb,)), ((), ())), preferred_element_type=F32)


def gelu_slope(hidden):
    square = hidden * hidden
    tanh_val = jnp.tanh(root_coef * (hidden + cube_coef * square * hidden))
    half = 0.5 * (1.0 + tanh_val)
    slope = half + 0.5 * hidden * (1.0 - tanh_val * tanh_val) * root_coef * (
        1.0 + 3.0 * cube_coef * square
    )
    return hidden * half, slope


def kernel(
    capacity, n_x, n_y,
    tok_hbm, dy_hbm, routes_hbm, keep_hbm, comb_hbm, win_hbm, wout_hbm,
    gtok_ref, gcomb_ref, gin_ref, gout_ref,
    routes_ref, keep_ref, comb_ref, tok, dy, ptok, pdy, meta, pmeta, win, wout,
    sent, psent_x, psent_s, own, part_x, part_s,
    first_m, second_m, chosen_m, weighted_m, hg_buf, act_buf, tg_acc, gate_acc, back_out, back_in,
    far_term, far_got, slope_pre, act_pre, term, got,
    load_sem, pair_send, pair_recv,
    lane_send, lane_recv, ring_send, ring_recv, far_send, far_recv,
):
    me = lax.axis_index("expert")
    z = lax.axis_index("dp")
    n_e = n_x * n_y * 2
    n_z = lax.axis_size("dp")
    toks, width = tok.shape
    rows = n_e * SLOT
    core, cx, cy = lax.rem(me, 2), lax.rem(me // 2, n_x), me // (2 * n_x)
    up, down = lax.rem(z + 1, n_z), lax.rem(z + n_z - 1, n_z)
    far = lax.rem(z + n_z // 2, n_z)

    barrier = pltpu.get_barrier_semaphore()
    for other in (far, up, down):
        pl.semaphore_signal(barrier, inc=1, device_id=(me, other), device_id_type=MESH)

    ahead_x = [lax.rem(cx + k, n_x) * 2 for k in range(n_x)]
    ahead_y = [lax.rem(cy + k, n_y) * (2 * n_x) for k in range(n_y)]
    cells = sorted(
        ((dx, dy_) for dx in range(n_x) for dy_ in range(n_y)),
        key=lambda cell: -min(cell[0], n_x - cell[0]) - min(cell[1], n_y - cell[1]),
    )
    peers = [
        ahead_y[dy_] + ahead_x[dx] + c
        for c in (1 - core, core) for dx, dy_ in cells
    ][:-1]
    for other in peers:
        pl.semaphore_signal(barrier, inc=1, device_id=(other, z), device_id_type=MESH)

    loads = [
        pltpu.make_async_copy(src, dst, load_sem.at[k])
        for k, (src, dst) in enumerate(
            (
                (tok_hbm, tok), (dy_hbm, dy), (win_hbm.at[0], win), (wout_hbm.at[0], wout),
                (routes_hbm, routes_ref), (keep_hbm, keep_ref), (comb_hbm, comb_ref),
            )
        )
    ]
    for k in (4, 5, 6, 0, 1, 2, 3):
        loads[k].start()

    for k in (4, 5, 6):
        loads[k].wait()
    expert_ids = lax.broadcasted_iota(jnp.int32, (n_e, toks), 0)
    r0, r1 = routes_ref[0:1, :], routes_ref[1:2, :]
    keep = keep_ref[...]
    first_hot = jnp.where(r0 == expert_ids, 1.0, 0.0)
    second_hot = jnp.where((r1 == expert_ids) & (keep > 0), 1.0, 0.0)
    earlier = jnp.where(
        lax.broadcasted_iota(jnp.int32, (toks, toks), 0)
        < lax.broadcasted_iota(jnp.int32, (toks, toks), 1), 1.0, 0.0,
    ).astype(BF16)
    first_pos = dot(first_hot.astype(BF16), earlier, 1, 0)
    second_pos = dot(second_hot.astype(BF16), earlier, 1, 0) + jnp.sum(
        first_hot, axis=1, keepdims=True
    )
    first_slot = jnp.sum(first_pos * first_hot, axis=0, keepdims=True)
    second_slot = jnp.sum(second_pos * second_hot, axis=0, keepdims=True)
    first_flat = jnp.where(first_slot < capacity, r0.astype(F32) * SLOT + first_slot, -1.0)
    second_flat = jnp.where(
        (keep > 0) & (second_slot < capacity), r1.astype(F32) * SLOT + second_slot, -1.0
    )
    weight = comb_ref[...].astype(F32)
    meta[0:1, :] = first_flat
    meta[1:2, :] = second_flat
    meta[2:4, :] = weight
    meta[4:8, :] = jnp.zeros((4, toks), F32)
    w0, w1 = weight[0:1, :], weight[1:2, :]
    slot_ids = lax.broadcasted_iota(jnp.int32, (rows, toks), 0).astype(F32)
    hit0, hit1 = slot_ids == first_flat, slot_ids == second_flat
    first_m[...] = jnp.where(hit0, 1.0, 0.0).astype(BF16)
    second_m[...] = jnp.where(hit1, 1.0, 0.0).astype(BF16)
    loads[0].wait()
    sent[:, 0] = dot(first_m[...] + second_m[...], tok[...], 1, 0).astype(BF16).reshape(
        n_e, SLOT, width
    )
    weighted = jnp.where(hit0, w0, 0.0) + jnp.where(hit1, w1, 0.0)
    loads[1].wait()
    sent[:, 1] = dot(weighted.astype(BF16), dy[...], 1, 0).astype(BF16).reshape(n_e, SLOT, width)

    pl.semaphore_wait(barrier, n_e + 2)

    cuts = [pl.ds(k * (width // PARTS), width // PARTS) for k in range(PARTS)]
    pair = [
        pltpu.make_async_remote_copy(
            src_ref=src, dst_ref=dst, send_sem=pair_send.at[k], recv_sem=pair_recv.at[k],
            device_id=(me, far), device_id_type=MESH,
        )
        for k, (src, dst) in enumerate(
            [(meta, pmeta)]
            + [(src.at[:, cut], dst.at[:, cut]) for src, dst in ((tok, ptok), (dy, pdy)) for cut in cuts]
        )
    ]
    for c in pair:
        c.start()

    lanes = ((sent, own), (back_out, back_in), (psent_x, part_x), (psent_s, part_s))
    last = len(lanes) - 2

    def hop(lane, src, dst, other, part=None):
        (left, right), sem = lanes[lane], lane
        left, right = left.at[src], right.at[dst]
        if part is not None:
            tail = (slice(None),) * (len(left.shape) - 1) + (cuts[part],)
            left, right = left.at[tail], right.at[tail]
            sem = last + (lane - last) * PARTS + part
        return pltpu.make_async_remote_copy(
            src_ref=left, dst_ref=right, send_sem=lane_send.at[sem], recv_sem=lane_recv.at[sem],
            device_id=(other, z), device_id_type=MESH,
        )

    def spread(lane, part=None):
        for other in peers:
            hop(lane, other, me, other, part).start()
        left, right = lanes[lane]
        if part is None:
            right[me] = left[me]
        else:
            right[me, :, cuts[part]] = left[me, :, cuts[part]]

    def whole(lane, part=None):
        return hop(lane, pl.ds(0, n_e - 1), pl.ds(0, n_e - 1), lax.rem(me + 1, n_e), part)

    spread(0)

    pair[0].wait_recv()
    p0, p1 = pmeta[0:1, :], pmeta[1:2, :]
    q0, q1 = pmeta[2:3, :], pmeta[3:4, :]
    chosen_m[...] = jnp.where((slot_ids == p0) | (slot_ids == p1), 1.0, 0.0).astype(BF16)
    weighted_m[...] = (
        jnp.where(slot_ids == p0, q0, 0.0) + jnp.where(slot_ids == p1, q1, 0.0)
    ).astype(BF16)

    def forward(lane, part):
        pair[1 + (lane - last) * PARTS + part].wait_recv()
        picks, source, out = ((chosen_m, ptok, psent_x), (weighted_m, pdy, psent_s))[lane - last]
        out[:, :, cuts[part]] = dot(picks[...], source[:, cuts[part]], 1, 0).astype(BF16).reshape(
            n_e, SLOT, width // PARTS
        )
        spread(lane, part)

    for part in range(PARTS):
        forward(2, part)

    ff_dev = gin_ref.shape[0]
    near_rows = ff_dev - LONG
    chunks = win.shape[0] // ff_dev
    loads[2].wait()
    loads[3].wait()
    whole(0).wait_recv()
    tg_acc[...] = jnp.zeros_like(tg_acc)
    gate_acc[...] = jnp.zeros_like(gate_acc)
    block, src = rows // 2, n_e // 2

    def own_chunk(j, carry):
        odd = lax.rem(j, 2)
        target = lax.rem(z + n_z // 2 + (1 - odd) * (j // 2) - odd * ((j + 1) // 2), n_z)
        cut = pl.ds(pl.multiple_of(target * ff_dev, ff_dev), ff_dev)
        for r in range(2):
            x_r = own[r * src:(r + 1) * src, 0].reshape(block, width)
            s_r = own[r * src:(r + 1) * src, 1].reshape(block, width)
            active, slope = gelu_slope(dot(x_r, win[cut, :], 1, 1))
            active_grad = dot(s_r, wout[cut, :], 1, 1)
            active = active.astype(BF16)
            hidden_grad = (active_grad * slope).astype(BF16)
            piece = pl.ds(r * block, block)
            act_buf[target, piece, :] = active
            hg_buf[target, piece, :] = hidden_grad
            product = active.astype(F32) * active_grad
            gate_acc[piece, :] += product[:, :GATE] + product[:, GATE:]
            tg_acc[piece, :] += dot(hidden_grad, win[cut, :], 1, 0)
        for m, left in enumerate((hg_buf, act_buf)):
            part = dot(
                left[target, :, ff_dev - 128:], own[:, m].reshape(rows, width), 0, 0
            )
            far_term[j, m] = part[128 - LONG:].astype(BF16)
        return carry

    def own_chunks(start, stop):
        lax.fori_loop(start, stop, own_chunk, 0)

    long_up = ((0, 0), (1, 1), (1, 0), (3, 1), (3, 0), (5, 1), (5, 0))
    long_down = ((0, 1), (2, 0), (2, 1), (4, 0), (4, 1), (6, 0), (6, 1))

    def long_hop(side, k):
        j, m = (long_up, long_down)[side][k]
        return pltpu.make_async_remote_copy(
            src_ref=far_term.at[j, m], dst_ref=far_got.at[side, k],
            send_sem=far_send.at[side, k], recv_sem=far_recv.at[side, k],
            device_id=(me, (up, down)[side]), device_id_type=MESH,
        )

    def relay(k):
        for side in range(2):
            j, m = (long_up, long_down)[side][k + 2]
            long_hop(side, k).wait_recv()
            far_term[j, m] = (far_term[j, m].astype(F32) + far_got[side, k].astype(F32)).astype(BF16)
            long_hop(side, k + 2).start()

    own_chunks(0, 3)
    for k in range(2):
        for side in range(2):
            long_hop(side, k).start()
    own_chunks(3, 4)
    forward(3, 0)
    own_chunks(4, 5)
    for part in range(1, PARTS):
        forward(3, part)

    own_chunks(5, 6)
    relay(0)
    own_chunks(6, 7)
    relay(1)
    own_chunks(7, 8)
    relay(2)
    back_out[:, :, :width] = tg_acc[...].astype(BF16).reshape(n_e, SLOT, width)
    gate = jnp.sum(gate_acc[...], axis=1, keepdims=True)
    back_out[:, :, width:] = jnp.broadcast_to(gate, (rows, GATE)).astype(BF16).reshape(
        n_e, SLOT, GATE
    )
    for part in range(PARTS):
        whole(2, part).wait_recv()
    above, below = lax.rem(z + 2, n_z), lax.rem(z + n_z - 2, n_z)

    def units(target):
        return pl.ds(pl.multiple_of(target * ff_dev, ff_dev), ff_dev)

    def rows_of(array):
        return array.reshape(rows, width)

    active, slope = gelu_slope(dot(rows_of(part_x[...]), win[units(above), :], 1, 1))
    slope_pre[...] = slope
    active, slope = gelu_slope(dot(rows_of(part_x[...]), win[units(below), :], 1, 1))
    act_pre[...] = active.astype(BF16)
    relay(3)
    gin_ref[...] = dot(hg_buf[above], rows_of(own[:, 0]), 0, 0)
    gout_ref[...] = dot(act_buf[below], rows_of(own[:, 1]), 0, 0)
    relay(4)
    for part in range(PARTS):
        whole(3, part).wait_recv()

    def near(target, store_in, store_out):
        x_p, s_p = rows_of(part_x[...]), rows_of(part_s[...])
        x_o, s_o = rows_of(own[:, 0]), rows_of(own[:, 1])
        active, slope = gelu_slope(dot(x_p, win[units(target), :], 1, 1))
        hidden_grad = (dot(s_p, wout[units(target), :], 1, 1) * slope).astype(BF16)
        grad = dot(hg_buf[target], x_o, 0, 0) + dot(hidden_grad, x_p, 0, 0)
        store_in(grad[:near_rows])
        grad = dot(act_buf[target], s_o, 0, 0) + dot(active.astype(BF16), s_p, 0, 0)
        store_out(grad[:near_rows])

    def ring(k):
        return pltpu.make_async_remote_copy(
            src_ref=term.at[k], dst_ref=got.at[k], send_sem=ring_send.at[k],
            recv_sem=ring_recv.at[k], device_id=(me, down if k % 2 else up), device_id_type=MESH,
        )

    def to_term(k):
        def store(grad):
            term[k] = grad.astype(BF16)

        return store

    def to_out(ref):
        def store(grad):
            ref[:near_rows, :] = grad

        return store

    grad = gout_ref[...] + dot(act_pre[...], rows_of(part_s[...]), 0, 0)
    to_term(1)(grad[:near_rows])
    ring(1).start()
    hidden_grad = (
        dot(rows_of(part_s[...]), wout[units(above), :], 1, 1) * slope_pre[...]
    ).astype(BF16)
    grad = gin_ref[...] + dot(hidden_grad, rows_of(part_x[...]), 0, 0)
    to_term(0)(grad[:near_rows])
    ring(0).start()
    spread(1)
    near(up, to_term(4), to_term(2))
    ring(2).start()
    near(down, to_term(3), to_term(5))
    ring(3).start()
    near(z, to_out(gin_ref), to_out(gout_ref))
    for m, (ref, k_up, k_down) in enumerate(((gin_ref, 6, 5), (gout_ref, 5, 6))):
        long_hop(0, k_up).wait_recv()
        long_hop(1, k_down).wait_recv()
        ref[near_rows:, :] = (
            far_term[chunks - 1, m].astype(F32)
            + far_got[0, k_up].astype(F32) + far_got[1, k_down].astype(F32)
        )
    for k in range(2):
        ring(k).wait_recv()
        term[4 + k] = (term[4 + k].astype(F32) + got[k].astype(F32)).astype(BF16)
        ring(4 + k).start()

    whole(1).wait_recv()
    back = back_in[...].reshape(rows, width + GATE)
    gtok_ref[...] = dot(first_m[...] + second_m[...], back[:, :width], 0, 0).astype(BF16)
    for k, hits in enumerate((first_m, second_m)):
        grad = dot(back[:, width:], hits[...], 0, 0)
        gcomb_ref[k:k + 1, :] = (grad[0:1, :] / meta[2 + k:3 + k, :]).astype(BF16)

    for k, ref in ((2, gout_ref), (3, gin_ref), (4, gin_ref), (5, gout_ref)):
        ring(k).wait_recv()
        ref[:near_rows, :] += got[k].astype(F32)

    for c in pair:
        c.wait_send()
    for lane in range(last):
        whole(lane).wait_send()
    for lane in range(last, len(lanes)):
        for part in range(PARTS):
            whole(lane, part).wait_send()
    for k in range(6):
        ring(k).wait_send()
    for side in range(2):
        for k in range(len(long_up)):
            long_hop(side, k).wait_send()


def hand_out(*refs):
    copies = [pltpu.make_async_copy(refs[k], refs[4 + k], refs[8].at[k]) for k in range(4)]
    for c in copies:
        c.start()
    for c in copies:
        c.wait()


def per_device(n_x, n_y, tokens, grad_out, routes, keep_second, combine, w_in, w_out):
    n_e = lax.axis_size("expert")
    toks, width = tokens.shape
    ff = w_in.shape[1]
    ff_dev = ff // lax.axis_size("dp")
    capacity = 5 * toks // (2 * n_e)
    rows = n_e * SLOT
    any_spec = pl.BlockSpec(memory_space=pltpu.HBM)
    vmem_spec = pl.BlockSpec(memory_space=pltpu.VMEM)
    slots = pltpu.VMEM((n_e, SLOT, width), BF16)
    pairs = pltpu.VMEM((n_e, 2, SLOT, width), BF16)
    results = pl.pallas_call(
        functools.partial(kernel, capacity, n_x, n_y),
        out_shape=(
            pltpu.VMEM((toks, width), BF16),
            pltpu.VMEM((2, toks), BF16),
            pltpu.VMEM((ff_dev, width), F32),
            pltpu.VMEM((ff_dev, width), F32),
        ),
        in_specs=[any_spec] * 7,
        out_specs=(vmem_spec,) * 4,
        scratch_shapes=[pltpu.VMEM((2, toks), jnp.int32), pltpu.VMEM((1, toks), jnp.int32)]
        + [pltpu.VMEM((2, toks), BF16)]
        + [pltpu.VMEM((toks, width), BF16)] * 4
        + [pltpu.VMEM((8, toks), F32)] * 2
        + [pltpu.VMEM((ff, width), BF16)] * 2
        + [pairs, slots, slots, pairs, slots, slots]
        + [pltpu.VMEM((rows, toks), BF16)] * 4
        + [pltpu.VMEM((ff // ff_dev, rows, ff_dev), BF16)] * 2
        + [pltpu.VMEM((rows, width), F32), pltpu.VMEM((rows, GATE), F32)]
        + [pltpu.VMEM((n_e, SLOT, width + GATE), BF16)] * 2
        + [pltpu.VMEM((ff // ff_dev, 2, LONG, width), BF16), pltpu.VMEM((2, 7, LONG, width), BF16)]
        + [pltpu.VMEM((rows, ff_dev), F32), pltpu.VMEM((rows, ff_dev), BF16)]
        + [pltpu.VMEM((6, ff_dev - LONG, width), BF16)] * 2
        + [pltpu.SemaphoreType.DMA((7,))]
        + [pltpu.SemaphoreType.DMA((1 + 2 * PARTS,))] * 2
        + [pltpu.SemaphoreType.DMA((2 + 2 * PARTS,))] * 2
        + [pltpu.SemaphoreType.DMA((6,))] * 2
        + [pltpu.SemaphoreType.DMA((2, 7))] * 2,
        compiler_params=pltpu.CompilerParams(
            collective_id=0, has_side_effects=True, vmem_limit_bytes=58 * 2**20
        ),
    )(
        tokens, grad_out, routes.T, keep_second.reshape(1, toks), combine.T, w_in, w_out,
    )
    gtok, gcomb, gin, gout = pl.pallas_call(
        hand_out,
        out_shape=tuple(jax.ShapeDtypeStruct(r.shape, r.dtype) for r in results),
        in_specs=[vmem_spec] * 4,
        out_specs=(any_spec,) * 4,
        scratch_shapes=[pltpu.SemaphoreType.DMA((4,))],
        compiler_params=pltpu.CompilerParams(vmem_limit_bytes=8 * 2**20),
    )(*results)
    return gtok, gcomb.T, gin[None], gout[None]


def solution(mesh):
    n_e = mesh.shape["expert"]
    n_x = 4
    return jax.shard_map(
        functools.partial(per_device, n_x, n_e // (2 * n_x)),
        mesh=mesh,
        in_specs=(
            P(("expert", "dp"), None),
            P(("expert", "dp"), None),
            P(("expert", "dp"), None),
            P(("expert", "dp")),
            P(("expert", "dp"), None),
            P("expert", None, None),
            P("expert", None, None),
        ),
        out_specs=(
            P(("expert", "dp"), None),
            P(("expert", "dp"), None),
            P("expert", "dp", None),
            P("expert", "dp", None),
        ),
        check_vma=False,
    )
```

```python
import functools

import jax
import jax.numpy as jnp
from jax import lax
from jax.experimental import pallas as pl
from jax.experimental.pallas import tpu as pltpu
from jax.sharding import PartitionSpec as P

MESH = pl.DeviceIdType.MESH
F32, BF16 = jnp.float32, jnp.bfloat16
root_coef = 0.7978845608
cube_coef = 0.044715
SLOT = 16
GATE = 128
PARTS = 2
LONG = 32


def dot(a, b, ca, cb):
    return lax.dot_general(a, b, (((ca,), (cb,)), ((), ())), preferred_element_type=F32)


def gelu_slope(hidden):
    square = hidden * hidden
    tanh_val = jnp.tanh(root_coef * (hidden + cube_coef * square * hidden))
    half = 0.5 * (1.0 + tanh_val)
    slope = half + 0.5 * hidden * (1.0 - tanh_val * tanh_val) * root_coef * (
        1.0 + 3.0 * cube_coef * square
    )
    return hidden * half, slope


def kernel(
    capacity, n_x, n_y,
    tok_hbm, dy_hbm, routes_hbm, keep_hbm, comb_hbm, win_hbm, wout_hbm,
    gtok_ref, gcomb_ref, gin_ref, gout_ref,
    routes_ref, keep_ref, comb_ref, tok, dy, ptok, pdy, meta, pmeta, win, wout,
    sent, psent_x, psent_s, own, part_x, part_s,
    first_m, second_m, chosen_m, weighted_m, hg_buf, act_buf, tg_acc, gate_acc, back_out, back_in,
    far_term, far_got, slope_pre, act_pre, grad_pre, term, got,
    load_sem, pair_send, pair_recv,
    lane_send, lane_recv, ring_send, ring_recv, far_send, far_recv,
):
    me = lax.axis_index("expert")
    z = lax.axis_index("dp")
    n_e = n_x * n_y * 2
    n_z = lax.axis_size("dp")
    toks, width = tok.shape
    rows = n_e * SLOT
    core, cx, cy = lax.rem(me, 2), lax.rem(me // 2, n_x), me // (2 * n_x)
    up, down = lax.rem(z + 1, n_z), lax.rem(z + n_z - 1, n_z)
    far = lax.rem(z + n_z // 2, n_z)

    loads = [
        pltpu.make_async_copy(src, dst, load_sem.at[k])
        for k, (src, dst) in enumerate(
            (
                (tok_hbm, tok), (dy_hbm, dy), (win_hbm.at[0], win), (wout_hbm.at[0], wout),
                (routes_hbm, routes_ref), (keep_hbm, keep_ref), (comb_hbm, comb_ref),
            )
        )
    ]
    for k in (4, 5, 6, 0, 1):
        loads[k].start()

    barrier = pltpu.get_barrier_semaphore()
    for other in (far, up, down):
        pl.semaphore_signal(barrier, inc=1, device_id=(me, other), device_id_type=MESH)

    ahead_x = [lax.rem(cx + k, n_x) * 2 for k in range(n_x)]
    ahead_y = [lax.rem(cy + k, n_y) * (2 * n_x) for k in range(n_y)]
    cells = (
        (2, 2), (1, 2), (2, 1), (2, 3), (3, 2), (2, 0), (1, 1), (1, 3),
        (0, 2), (3, 1), (3, 3), (1, 0), (0, 1), (0, 3), (3, 0), (0, 0),
    )
    assert n_x == n_y == 4
    peers = [
        ahead_y[dy_] + ahead_x[dx] + c
        for c in (1 - core, core) for dx, dy_ in cells
    ][:-1]
    for other in peers:
        pl.semaphore_signal(barrier, inc=1, device_id=(other, z), device_id_type=MESH)

    for k in (2, 3):
        loads[k].start()

    for k in (4, 5, 6):
        loads[k].wait()
    expert_ids = lax.broadcasted_iota(jnp.int32, (n_e, toks), 0)
    r0, r1 = routes_ref[0:1, :], routes_ref[1:2, :]
    keep = keep_ref[...]
    first_hot = jnp.where(r0 == expert_ids, 1.0, 0.0)
    second_hot = jnp.where((r1 == expert_ids) & (keep > 0), 1.0, 0.0)
    earlier = jnp.where(
        lax.broadcasted_iota(jnp.int32, (toks, toks), 0)
        < lax.broadcasted_iota(jnp.int32, (toks, toks), 1), 1.0, 0.0,
    ).astype(BF16)
    first_pos = dot(first_hot.astype(BF16), earlier, 1, 0)
    second_pos = dot(second_hot.astype(BF16), earlier, 1, 0) + jnp.sum(
        first_hot, axis=1, keepdims=True
    )
    first_slot = jnp.sum(first_pos * first_hot, axis=0, keepdims=True)
    second_slot = jnp.sum(second_pos * second_hot, axis=0, keepdims=True)
    first_flat = jnp.where(first_slot < capacity, r0.astype(F32) * SLOT + first_slot, -1.0)
    second_flat = jnp.where(
        (keep > 0) & (second_slot < capacity), r1.astype(F32) * SLOT + second_slot, -1.0
    )
    weight = comb_ref[...].astype(F32)
    meta[0:1, :] = first_flat
    meta[1:2, :] = second_flat
    meta[2:4, :] = weight
    meta[4:8, :] = jnp.zeros((4, toks), F32)
    w0, w1 = weight[0:1, :], weight[1:2, :]
    slot_ids = lax.broadcasted_iota(jnp.int32, (rows, toks), 0).astype(F32)
    hit0, hit1 = slot_ids == first_flat, slot_ids == second_flat
    first_m[...] = jnp.where(hit0, 1.0, 0.0).astype(BF16)
    second_m[...] = jnp.where(hit1, 1.0, 0.0).astype(BF16)
    loads[0].wait()
    sent[:, 0] = dot(first_m[...] + second_m[...], tok[...], 1, 0).astype(BF16).reshape(
        n_e, SLOT, width
    )
    weighted = jnp.where(hit0, w0, 0.0) + jnp.where(hit1, w1, 0.0)
    loads[1].wait()
    sent[:, 1] = dot(weighted.astype(BF16), dy[...], 1, 0).astype(BF16).reshape(n_e, SLOT, width)

    pl.semaphore_wait(barrier, n_e + 2)

    cuts = [pl.ds(k * (width // PARTS), width // PARTS) for k in range(PARTS)]
    pair = [
        pltpu.make_async_remote_copy(
            src_ref=src, dst_ref=dst, send_sem=pair_send.at[k], recv_sem=pair_recv.at[k],
            device_id=(me, far), device_id_type=MESH,
        )
        for k, (src, dst) in enumerate(
            [(meta, pmeta)]
            + [(src.at[:, cut], dst.at[:, cut]) for src, dst in ((tok, ptok), (dy, pdy)) for cut in cuts]
        )
    ]
    for c in pair:
        c.start()

    lanes = ((sent, own), (back_out, back_in), (psent_x, part_x), (psent_s, part_s))
    last = len(lanes) - 2

    def hop(lane, src, dst, other, part=None):
        (left, right), sem = lanes[lane], lane
        left, right = left.at[src], right.at[dst]
        if part is not None:
            tail = (slice(None),) * (len(left.shape) - 1) + (cuts[part],)
            left, right = left.at[tail], right.at[tail]
            sem = last + (lane - last) * PARTS + part
        return pltpu.make_async_remote_copy(
            src_ref=left, dst_ref=right, send_sem=lane_send.at[sem], recv_sem=lane_recv.at[sem],
            device_id=(other, z), device_id_type=MESH,
        )

    def spread(lane, part=None):
        for other in peers:
            hop(lane, other, me, other, part).start()
        left, right = lanes[lane]
        if part is None:
            right[me] = left[me]
        else:
            right[me, :, cuts[part]] = left[me, :, cuts[part]]

    def whole(lane, part=None):
        return hop(lane, pl.ds(0, n_e - 1), pl.ds(0, n_e - 1), lax.rem(me + 1, n_e), part)

    spread(0)

    pair[0].wait_recv()
    p0, p1 = pmeta[0:1, :], pmeta[1:2, :]
    q0, q1 = pmeta[2:3, :], pmeta[3:4, :]
    chosen_m[...] = jnp.where((slot_ids == p0) | (slot_ids == p1), 1.0, 0.0).astype(BF16)
    weighted_m[...] = (
        jnp.where(slot_ids == p0, q0, 0.0) + jnp.where(slot_ids == p1, q1, 0.0)
    ).astype(BF16)

    def forward(lane, part):
        pair[1 + (lane - last) * PARTS + part].wait_recv()
        picks, source, out = ((chosen_m, ptok, psent_x), (weighted_m, pdy, psent_s))[lane - last]
        out[:, :, cuts[part]] = dot(picks[...], source[:, cuts[part]], 1, 0).astype(BF16).reshape(
            n_e, SLOT, width // PARTS
        )
        spread(lane, part)

    for part in range(PARTS):
        forward(2, part)

    ff_dev = gin_ref.shape[0]
    near_rows = ff_dev - LONG
    chunks = win.shape[0] // ff_dev
    loads[2].wait()
    loads[3].wait()
    whole(0).wait_recv()
    tg_acc[...] = jnp.zeros_like(tg_acc)
    gate_acc[...] = jnp.zeros_like(gate_acc)
    block, src = rows // 2, n_e // 2

    def own_chunk(j, carry):
        odd = lax.rem(j, 2)
        target = lax.rem(z + n_z // 2 + (1 - odd) * (j // 2) - odd * ((j + 1) // 2), n_z)
        cut = pl.ds(pl.multiple_of(target * ff_dev, ff_dev), ff_dev)
        for r in range(2):
            x_r = own[r * src:(r + 1) * src, 0].reshape(block, width)
            s_r = own[r * src:(r + 1) * src, 1].reshape(block, width)
            active, slope = gelu_slope(dot(x_r, win[cut, :], 1, 1))
            active_grad = dot(s_r, wout[cut, :], 1, 1)
            active = active.astype(BF16)
            hidden_grad = (active_grad * slope).astype(BF16)
            piece = pl.ds(r * block, block)
            act_buf[target, piece, :] = active
            hg_buf[target, piece, :] = hidden_grad
            product = active.astype(F32) * active_grad
            gate_acc[piece, :] += product[:, :GATE] + product[:, GATE:]
            tg_acc[piece, :] += dot(hidden_grad, win[cut, :], 1, 0)
        for m, left in enumerate((hg_buf, act_buf)):
            part = dot(
                left[target, :, ff_dev - 128:], own[:, m].reshape(rows, width), 0, 0
            )
            far_term[j, m] = part[128 - LONG:].astype(BF16)
        return carry

    def own_chunks(start, stop):
        lax.fori_loop(start, stop, own_chunk, 0)

    long_up = ((0, 0), (1, 1), (1, 0), (3, 1), (3, 0), (5, 1), (5, 0))
    long_down = ((0, 1), (2, 0), (2, 1), (4, 0), (4, 1), (6, 0), (6, 1))

    def long_hop(side, k):
        j, m = (long_up, long_down)[side][k]
        return pltpu.make_async_remote_copy(
            src_ref=far_term.at[j, m], dst_ref=far_got.at[side, k],
            send_sem=far_send.at[side, k], recv_sem=far_recv.at[side, k],
            device_id=(me, (up, down)[side]), device_id_type=MESH,
        )

    def relay(k):
        for side in range(2):
            j, m = (long_up, long_down)[side][k + 2]
            long_hop(side, k).wait_recv()
            far_term[j, m] = (far_term[j, m].astype(F32) + far_got[side, k].astype(F32)).astype(BF16)
            long_hop(side, k + 2).start()

    own_chunks(0, 3)
    for k in range(2):
        for side in range(2):
            long_hop(side, k).start()
    own_chunks(3, 4)
    forward(3, 0)
    own_chunks(4, 5)
    for part in range(1, PARTS):
        forward(3, part)

    own_chunks(5, 6)
    relay(0)
    own_chunks(6, 7)
    relay(1)
    own_chunks(7, 8)
    relay(2)
    back_out[:, :, :width] = tg_acc[...].astype(BF16).reshape(n_e, SLOT, width)
    gate = jnp.sum(gate_acc[...], axis=1, keepdims=True)
    back_out[:, :, width:] = jnp.broadcast_to(gate, (rows, GATE)).astype(BF16).reshape(
        n_e, SLOT, GATE
    )
    for part in range(PARTS):
        whole(2, part).wait_recv()
    above, below = lax.rem(z + 2, n_z), lax.rem(z + n_z - 2, n_z)

    def units(target):
        return pl.ds(pl.multiple_of(target * ff_dev, ff_dev), ff_dev)

    def rows_of(array):
        return array.reshape(rows, width)

    active, slope = gelu_slope(dot(rows_of(part_x[...]), win[units(above), :], 1, 1))
    slope_pre[...] = slope
    active, slope = gelu_slope(dot(rows_of(part_x[...]), win[units(below), :], 1, 1))
    act_pre[...] = active.astype(BF16)
    relay(3)
    gin_ref[...] = dot(hg_buf[above], rows_of(own[:, 0]), 0, 0)
    gout_ref[...] = dot(act_buf[below], rows_of(own[:, 1]), 0, 0)
    def take(part):
        whole(3, part).wait_recv()
        block_s = part_s[:, :, cuts[part]].reshape(rows, width // PARTS)
        gout_ref[:, cuts[part]] += dot(act_pre[...], block_s, 0, 0)
        return dot(block_s, wout[units(above), cuts[part]], 1, 1)

    grad_pre[...] = take(0)
    for part in range(1, PARTS - 1):
        grad_pre[...] += take(part)
    relay(4)
    active_grad = take(PARTS - 1) + grad_pre[...]

    def near(target, store_in, store_out):
        x_p, s_p = rows_of(part_x[...]), rows_of(part_s[...])
        x_o, s_o = rows_of(own[:, 0]), rows_of(own[:, 1])
        active, slope = gelu_slope(dot(x_p, win[units(target), :], 1, 1))
        hidden_grad = (dot(s_p, wout[units(target), :], 1, 1) * slope).astype(BF16)
        grad = dot(hg_buf[target], x_o, 0, 0) + dot(hidden_grad, x_p, 0, 0)
        store_in(grad[:near_rows])
        grad = dot(act_buf[target], s_o, 0, 0) + dot(active.astype(BF16), s_p, 0, 0)
        store_out(grad[:near_rows])

    def ring(k):
        return pltpu.make_async_remote_copy(
            src_ref=term.at[k], dst_ref=got.at[k], send_sem=ring_send.at[k],
            recv_sem=ring_recv.at[k], device_id=(me, down if k % 2 else up), device_id_type=MESH,
        )

    def to_term(k):
        def store(grad):
            term[k] = grad.astype(BF16)

        return store

    def to_out(ref):
        def store(grad):
            ref[:near_rows, :] = grad

        return store

    to_term(1)(gout_ref[:near_rows, :])
    ring(1).start()
    hidden_grad = (active_grad * slope_pre[...]).astype(BF16)
    grad = gin_ref[...] + dot(hidden_grad, rows_of(part_x[...]), 0, 0)
    to_term(0)(grad[:near_rows])
    ring(0).start()
    spread(1)
    near(up, to_term(4), to_term(2))
    ring(2).start()
    near(down, to_term(3), to_term(5))
    ring(3).start()
    near(z, to_out(gin_ref), to_out(gout_ref))
    for m, (ref, k_up, k_down) in enumerate(((gin_ref, 6, 5), (gout_ref, 5, 6))):
        long_hop(0, k_up).wait_recv()
        long_hop(1, k_down).wait_recv()
        ref[near_rows:, :] = (
            far_term[chunks - 1, m].astype(F32)
            + far_got[0, k_up].astype(F32) + far_got[1, k_down].astype(F32)
        )
    for k in range(2):
        ring(k).wait_recv()
        term[4 + k] = (term[4 + k].astype(F32) + got[k].astype(F32)).astype(BF16)
        ring(4 + k).start()

    whole(1).wait_recv()
    back = back_in[...].reshape(rows, width + GATE)
    gtok_ref[...] = dot(first_m[...] + second_m[...], back[:, :width], 0, 0).astype(BF16)
    for k, hits in enumerate((first_m, second_m)):
        grad = dot(back[:, width:], hits[...], 0, 0)
        gcomb_ref[k:k + 1, :] = (grad[0:1, :] / meta[2 + k:3 + k, :]).astype(BF16)

    for k, ref in ((2, gout_ref), (3, gin_ref), (4, gin_ref), (5, gout_ref)):
        ring(k).wait_recv()
        ref[:near_rows, :] += got[k].astype(F32)

    for c in pair:
        c.wait_send()
    for lane in range(last):
        whole(lane).wait_send()
    for lane in range(last, len(lanes)):
        for part in range(PARTS):
            whole(lane, part).wait_send()
    for k in range(6):
        ring(k).wait_send()
    for side in range(2):
        for k in range(len(long_up)):
            long_hop(side, k).wait_send()


def hand_out(*refs):
    copies = [pltpu.make_async_copy(refs[k], refs[4 + k], refs[8].at[k]) for k in range(4)]
    for c in copies:
        c.start()
    for c in copies:
        c.wait()


def per_device(n_x, n_y, tokens, grad_out, routes, keep_second, combine, w_in, w_out):
    n_e = lax.axis_size("expert")
    toks, width = tokens.shape
    ff = w_in.shape[1]
    ff_dev = ff // lax.axis_size("dp")
    capacity = 5 * toks // (2 * n_e)
    rows = n_e * SLOT
    any_spec = pl.BlockSpec(memory_space=pltpu.HBM)
    vmem_spec = pl.BlockSpec(memory_space=pltpu.VMEM)
    slots = pltpu.VMEM((n_e, SLOT, width), BF16)
    pairs = pltpu.VMEM((n_e, 2, SLOT, width), BF16)
    results = pl.pallas_call(
        functools.partial(kernel, capacity, n_x, n_y),
        out_shape=(
            pltpu.VMEM((toks, width), BF16),
            pltpu.VMEM((2, toks), BF16),
            pltpu.VMEM((ff_dev, width), F32),
            pltpu.VMEM((ff_dev, width), F32),
        ),
        in_specs=[any_spec] * 7,
        out_specs=(vmem_spec,) * 4,
        scratch_shapes=[pltpu.VMEM((2, toks), jnp.int32), pltpu.VMEM((1, toks), jnp.int32)]
        + [pltpu.VMEM((2, toks), BF16)]
        + [pltpu.VMEM((toks, width), BF16)] * 4
        + [pltpu.VMEM((8, toks), F32)] * 2
        + [pltpu.VMEM((ff, width), BF16)] * 2
        + [pairs, slots, slots, pairs, slots, slots]
        + [pltpu.VMEM((rows, toks), BF16)] * 4
        + [pltpu.VMEM((ff // ff_dev, rows, ff_dev), BF16)] * 2
        + [pltpu.VMEM((rows, width), F32), pltpu.VMEM((rows, GATE), F32)]
        + [pltpu.VMEM((n_e, SLOT, width + GATE), BF16)] * 2
        + [pltpu.VMEM((ff // ff_dev, 2, LONG, width), BF16), pltpu.VMEM((2, 7, LONG, width), BF16)]
        + [pltpu.VMEM((rows, ff_dev), F32), pltpu.VMEM((rows, ff_dev), BF16), pltpu.VMEM((rows, ff_dev), F32)]
        + [pltpu.VMEM((6, ff_dev - LONG, width), BF16)] * 2
        + [pltpu.SemaphoreType.DMA((7,))]
        + [pltpu.SemaphoreType.DMA((1 + 2 * PARTS,))] * 2
        + [pltpu.SemaphoreType.DMA((2 + 2 * PARTS,))] * 2
        + [pltpu.SemaphoreType.DMA((6,))] * 2
        + [pltpu.SemaphoreType.DMA((2, 7))] * 2,
        compiler_params=pltpu.CompilerParams(
            collective_id=0, has_side_effects=True, vmem_limit_bytes=58 * 2**20
        ),
    )(
        tokens, grad_out, routes.T, keep_second.reshape(1, toks), combine.T, w_in, w_out,
    )
    gtok, gcomb, gin, gout = pl.pallas_call(
        hand_out,
        out_shape=tuple(jax.ShapeDtypeStruct(r.shape, r.dtype) for r in results),
        in_specs=[vmem_spec] * 4,
        out_specs=(any_spec,) * 4,
        scratch_shapes=[pltpu.SemaphoreType.DMA((4,))],
        compiler_params=pltpu.CompilerParams(vmem_limit_bytes=8 * 2**20),
    )(*results)
    return gtok, gcomb.T, gin[None], gout[None]


def solution(mesh):
    n_e = mesh.shape["expert"]
    n_x = 4
    return jax.shard_map(
        functools.partial(per_device, n_x, n_e // (2 * n_x)),
        mesh=mesh,
        in_specs=(
            P(("expert", "dp"), None),
            P(("expert", "dp"), None),
            P(("expert", "dp"), None),
            P(("expert", "dp")),
            P(("expert", "dp"), None),
            P("expert", None, None),
            P("expert", None, None),
        ),
        out_specs=(
            P(("expert", "dp"), None),
            P(("expert", "dp"), None),
            P("expert", "dp", None),
            P("expert", "dp", None),
        ),
        check_vma=False,
    )
```
